1024 devices in a mesh: gx: 8 (over z_lo), gy: 16 (over y, z_hi), gz: 8 (over x, core).
Axes of the slice: x: 4, y: 8, z: 16 (z_hi: 2, z_lo: 8; z = z_hi * 8 + z_lo), core: 2. Of those that a mesh axis runs over, the one named last changes fastest.
Arguments:
- coefficients: bfloat16 [64, 256, 128, 128], P('gx', 'gy', 'gz'), may hold values from -0.109375 to 0.109375
- potential: float32 [64, 256, 128], P('gx', 'gy', 'gz'), may hold values from 0.5 to 2
- owner_map: int32 [8, 16, 8, 7, 1], P('gx', 'gy', 'gz'), may hold values from 0 to 7; in each aligned block of 7 rows (0 to 6, 7 to 13, ..., all dimensions but the last counted through in order) at most 2 rows name the same one
Outputs:
- correction: bfloat16 [8, 16, 8, 16, 128, 128], P('gx', 'gy', 'gz')
The draws below stay inside these ranges and needn't reach their ends.
Inputs may be any that keep to these rules, and one draw needn't show every extreme that they name: `owner_map`: among the 7 blocks of one subdomain no owner is named more than 2 times; in every draw some subdomain names some owner exactly 2 times.
All inputs are finite; a program needn't handle non-finite values.
Results may differ from the reference program's by a relative error of at most 0.0062.
Values may be sent and summed in bfloat16 or wider, within the bound.
A program may use at most 32 MiB of HBM per device.

```python
import math
import jax
import jax.numpy as jnp
import numpy as np
from jax import lax

NORB = 128
CX = 8
CY = 16
CZ = 16
BLOCKS = 7
CAP = 2
NX = 64
NY = 256
NZ = 128
N_GX = 8
N_GY = 16
N_GZ = 8


def shard_levels(own_key, shape, cuts, low, largest):
    factor_of, own = 1.0, jax.random.fold_in(own_key, 6)
    for dim, blocks in cuts:
        steps = jnp.exp(jax.random.uniform(jax.random.fold_in(own, dim), (blocks,), jnp.float32, low / len(cuts), largest / len(cuts)))
        factor_of = factor_of * jnp.repeat(steps, shape[dim] // blocks).reshape([-1 if axis == dim else 1 for axis in range(len(shape))])
    return factor_of


def assign_block(own_key, own, number, rows, amount, top, limit, lean):
    sequence = jax.random.permutation(own_key, amount)
    crowded, usual = shares(amount, rows * top, limit, lean, True), shares(amount, rows * top, limit, lean, False)
    places = jnp.arange(amount)

    def named(sizes, rotation):
        used = int((sizes > 0).sum())
        fixed = max(1, used // 4)
        moved = fixed + (places - fixed + rotation * (used - fixed)) % max(1, amount - fixed)
        return jnp.zeros((amount,), jnp.int32).at[sequence[jnp.where(places < fixed, places, moved)]].set(jnp.asarray(sizes, jnp.int32))

    sizes = jnp.where(number % 4 == 0, named(crowded, number // 4), named(usual, number - number // 4 - 1))
    mixed = jax.random.permutation(jax.random.fold_in(own, 3), amount)
    donor, taker = mixed[0:amount // 2 * 2:2], mixed[1:amount // 2 * 2:2]
    room = jnp.minimum(sizes[donor] - 1, limit - sizes[taker]) // 2
    room = jnp.where((donor == sequence[0]) | (taker == sequence[0]) | (sizes[taker] == 0), 0, jnp.maximum(room, 0))
    moved = jax.random.randint(jax.random.fold_in(own, 4), (amount // 2,), 0, 1 << 20) % (room + 1)
    sizes = sizes.at[donor].add(-moved).at[taker].add(moved)
    labels = jnp.searchsorted(jnp.cumsum(sizes), jnp.arange(rows * top), side="right").astype(jnp.int32)
    listing = labels.reshape(top, rows).T
    listing = listing[jax.random.permutation(jax.random.fold_in(own, 1), rows)]
    rotation = jax.random.randint(jax.random.fold_in(own, 2), (rows, 1), 0, top)
    return jnp.take_along_axis(listing, (jnp.arange(top)[None, :] + rotation) % top, axis=1)


def shares(count, total, bound, lean, full):
    weights = [(1 << 20) // math.isqrt(rank ** lean) + 1 for rank in range(1, count + 1)]
    largest = bound if full else min(bound, max(-(-total // count), total * weights[0] // sum(weights)))
    least = 1 if total - largest >= count - 1 else 0
    counts, rest = [largest] + [least] * (count - 1), total - largest - least * (count - 1)
    while rest > 0:
        candidates = [i for i in range(1, count) if counts[i] < largest] or [i for i in range(1, count) if counts[i] < bound]
        pool, remaining = sum([weights[i] for i in candidates]), rest
        for i in candidates:
            more = min(bound - counts[i], max(1, remaining * weights[i] // pool), rest)
            counts[i] = counts[i] + more
            rest = rest - more
    return np.array(counts)


def scatter_about(rng, shape, scale, reach, split=(), kind=jnp.bfloat16):
    drawn = jax.random.normal(rng, shape, jnp.float32) * scale
    if len(split) > 0:
        drawn = shard_levels(rng, shape, split, -0.22, 0.18) * drawn
    return jnp.clip(drawn, min=-reach, max=reach).astype(kind)


def setup_inputs(seed: int = 0) -> dict:
    splits = jax.random.split(jax.random.key(seed), 4)
    coefficients = scatter_about(splits[0], (NX, NY, NZ, NORB), (CX * CY * CZ * 1.375) ** -0.5, 0.109375, ((0, 8), (1, 16), (2, 8)))
    potential = jnp.clip(0.5 + 1.5 * jax.random.uniform(splits[1], (NX, NY, NZ), jnp.float32) ** shard_levels(splits[1], (NX, NY, NZ), ((0, 8), (1, 16), (2, 8)), -0.2, 0.2), 0.5, 2.0)
    owner_map_keys = jax.random.split(jax.random.fold_in(splits[2], 1), N_GX * N_GY * N_GZ * BLOCKS // BLOCKS)
    owner_map_turns = jax.random.permutation(jax.random.fold_in(splits[2], 3), N_GX * N_GY * N_GZ * BLOCKS // BLOCKS)
    owner_map = jax.vmap(lambda own, number: assign_block(jax.random.fold_in(splits[2], 2), own, number, BLOCKS, N_GX, 1, CAP, 2))(owner_map_keys, owner_map_turns).reshape((N_GX, N_GY, N_GZ, BLOCKS, 1))
    return dict(coefficients=coefficients, potential=potential, owner_map=owner_map)


SMOOTH = 0.25


def moved(field, dim, step):
    count = field.shape[dim]
    zero = jnp.zeros_like(lax.slice_in_dim(field, 0, 1, axis=dim))
    if step > 0:
        return jnp.concatenate([lax.slice_in_dim(field, 1, count, axis=dim), zero], axis=dim)
    return jnp.concatenate([zero, lax.slice_in_dim(field, 0, count - 1, axis=dim)], axis=dim)


def neighbour_sum(field, dims):
    total = jnp.zeros(field.shape, jnp.float32)
    for dim in dims:
        total = total + moved(field, dim, 1).astype(jnp.float32) + moved(field, dim, -1).astype(jnp.float32)
    return total


def gram(left, right):
    width = left.shape[-1]
    return jnp.dot(left.reshape(-1, width).T, right.reshape(-1, right.shape[-1]), preferred_element_type=jnp.float32)


def one_device(index, coefficients, potential):
    first = (index // (N_GY * N_GZ)).astype(jnp.int32)
    second = ((index // N_GZ) % N_GY).astype(jnp.int32)
    third = (index % N_GZ).astype(jnp.int32)
    cells = (CX, CY, CZ)
    whole = (NX, NY, NZ)
    place = (first, second, third)
    starts = [(first * CX).astype(jnp.int32), (second * CY).astype(jnp.int32), (third * CZ).astype(jnp.int32)]
    zero = jnp.zeros((), jnp.int32)
    block = lax.dynamic_slice(coefficients, (starts[0], starts[1], starts[2], zero), (CX, CY, CZ, NORB))
    local_pot = lax.dynamic_slice(potential, (starts[0], starts[1], starts[2]), (CX, CY, CZ))
    smooth = (block.astype(jnp.float32) + SMOOTH * neighbour_sum(block, (0, 1, 2))).astype(jnp.bfloat16)
    weighted = (local_pot[..., None] * smooth.astype(jnp.float32)).astype(jnp.bfloat16)
    hamilton = gram(smooth, weighted).astype(jnp.bfloat16)
    correlation = gram(smooth, smooth)
    faces = []
    for dim in range(3):
        lateral = tuple(other for other in range(3) if other != dim)
        size = cells[dim]
        for side in (-1, 1):
            edge = 0 if side < 0 else size - 1
            c_own = lax.slice_in_dim(block, edge, edge + 1, axis=dim)
            s_own = lax.slice_in_dim(smooth, edge, edge + 1, axis=dim)
            if side > 0:
                begin = ((place[dim] + 1) * size) % whole[dim]
            else:
                begin = (place[dim] * size - 2 + whole[dim]) % whole[dim]
            begins = list(starts) + [zero]
            begins[dim] = begin.astype(jnp.int32)
            extent = [CX, CY, CZ, NORB]
            extent[dim] = 2
            slab = lax.dynamic_slice(coefficients, tuple(begins), tuple(extent))
            far_at, deep_at = (0, 1) if side > 0 else (1, 0)
            c_far = lax.slice_in_dim(slab, far_at, far_at + 1, axis=dim)
            c_deep = lax.slice_in_dim(slab, deep_at, deep_at + 1, axis=dim)
            s_far = (c_far.astype(jnp.float32) + SMOOTH * (c_deep.astype(jnp.float32) + neighbour_sum(c_far, lateral))).astype(jnp.bfloat16)
            correlation = correlation + SMOOTH * SMOOTH * gram(c_own, c_own)
            faces.append(SMOOTH * (gram(s_own, c_far) + gram(c_own, s_far)))
    scale = jnp.float32((CX * CY * CZ) ** 0.5)
    blocks = jnp.stack([correlation - jnp.eye(NORB, dtype=jnp.float32)] + faces)
    deviation = (scale * blocks).astype(jnp.bfloat16)
    product = jnp.einsum("fab,bc->fac", deviation.astype(jnp.float32), hamilton.astype(jnp.float32)).astype(jnp.bfloat16)
    return product


def reference(coefficients, potential, owner_map):
    devices = N_GX * N_GY * N_GZ

    def for_device(index):
        return one_device(index, coefficients, potential)

    products = lax.map(for_device, jnp.arange(devices, dtype=jnp.int32))
    products = products.reshape(N_GX, N_GY, N_GZ, BLOCKS, NORB, NORB)
    routes = owner_map.reshape(N_GX, N_GY, N_GZ, BLOCKS)
    order = jnp.arange(BLOCKS, dtype=jnp.int32)
    same = routes[..., :, None] == routes[..., None, :]
    earlier = order[None, :] < order[:, None]
    rank = jnp.sum((same & earlier).astype(jnp.int32), axis=-1)
    slots = jnp.arange(CAP, dtype=jnp.int32)

    def for_owner(owner):
        pick = ((routes[..., None, :] == owner) & (rank[..., None, :] == slots[:, None])).astype(jnp.float32)
        placed = jnp.einsum("xyzsf,xyzfab->yzxsab", pick, products.astype(jnp.float32), precision=lax.Precision.HIGHEST)
        return placed.reshape(N_GY, N_GZ, N_GX * CAP, NORB, NORB).astype(jnp.bfloat16)

    return lax.map(for_owner, jnp.arange(N_GX, dtype=jnp.int32))
```

```python
import functools
import math

import jax
import jax.numpy as jnp
from jax import lax
from jax.experimental import pallas as pl
from jax.experimental.pallas import tpu as pltpu
from jax.sharding import PartitionSpec as P

CAP = 2
SMOOTH = 0.25
MESH = pl.DeviceIdType.MESH
F32 = jnp.float32
BF16 = jnp.bfloat16


def dot(a, b):
    return jnp.dot(a, b, preferred_element_type=F32)


def gram(a, b):
    return lax.dot_general(a, b, (((0,), (0,)), ((), ())), preferred_element_type=F32)


def kernel(
    sizes,
    c_hbm,
    pot_hbm,
    own_hbm,
    out,
    c_v,
    s_v,
    pot_v,
    own_s,
    sel_s,
    x_rx,
    y_rx,
    z_tx,
    z_own,
    z_rx,
    ret_tx,
    ret_rx,
    prod,
    slots,
    load_sem,
    tx_sem,
    rx_sem,
    a2a_tx,
    a2a_rx,
):
    n_x, n_y, n_z = sizes
    cx, cy, cz, orb = c_hbm.shape
    p, q, r = (lax.axis_index(a) for a in ("gx", "gy", "gz"))
    low = q % 2 == 0
    x_lo, x_hi = ((p + n_x - 1) % n_x, q, r), ((p + 1) % n_x, q, r)
    y_lo, y_hi = (p, (q + n_y - 1) % n_y, r), (p, (q + 1) % n_y, r)
    z_lo, z_hi = (p, q, (r + n_z - 1) % n_z), (p, q, (r + 1) % n_z)

    loads = [
        pltpu.make_async_copy(c_hbm, c_v, load_sem.at[0]),
        pltpu.make_async_copy(pot_hbm, pot_v, load_sem.at[1]),
        pltpu.make_async_copy(own_hbm, own_s, load_sem.at[2]),
    ]
    for load in loads:
        load.start()

    barrier = pltpu.get_barrier_semaphore()
    for k in range(1, n_x):
        pl.semaphore_signal(barrier, inc=1, device_id=((p + k) % n_x, q, r), device_id_type=MESH)
    for peer in (z_lo, z_hi):
        pl.semaphore_signal(barrier, inc=1, device_id=peer, device_id_type=MESH)

    @pl.when(low)
    def _():
        for peer in (y_lo, y_hi):
            pl.semaphore_signal(barrier, inc=1, device_id=peer, device_id_type=MESH)

    def send(src, dst, sem, peer):
        return pltpu.make_async_remote_copy(
            src_ref=src,
            dst_ref=dst,
            send_sem=tx_sem.at[sem],
            recv_sem=rx_sem.at[sem],
            device_id=peer,
            device_id_type=MESH,
        )

    push_x = send(c_v.at[pl.ds(cx - 2, 2)], x_rx, 0, x_hi)
    push_z = [send(z_tx.at[0], z_rx.at[1], 1, z_lo), send(z_tx.at[1], z_rx.at[0], 2, z_hi)]
    back_x = send(ret_tx.at[0], ret_rx.at[0], 3, x_lo)
    push_y = [
        send(c_v.at[:, pl.ds(0, 2)], y_rx.at[1], 4, y_lo),
        send(c_v.at[:, pl.ds(cy - 2, 2)], y_rx.at[0], 5, y_hi),
    ]
    back_y = [
        send(ret_tx.at[1], ret_rx.at[2], 6, y_lo),
        send(ret_tx.at[2], ret_rx.at[1], 7, y_hi),
    ]

    loads[0].wait()
    pl.semaphore_wait(barrier, jnp.where(low, n_x + 1, n_x + 3))

    @pl.when(jnp.logical_not(low))
    def _():
        for copy in push_y:
            copy.start()

    push_x.start()

    layer = cy * cz
    row = lax.broadcasted_iota(jnp.int32, (layer, layer), 0)
    col = lax.broadcasted_iota(jnp.int32, (layer, layer), 1)
    apart = jnp.abs(row - col)
    beside = ((apart == 1) & (row // cz == col // cz)) | (apart == cz)
    stencil = jnp.where(apart == 0, 1.0, jnp.where(beside, SMOOTH, 0.0)).astype(BF16)
    face = cx * cz
    small = stencil[:face, :face]

    pr = lax.broadcasted_iota(jnp.int32, (4 * cy, layer), 0)
    pc = lax.broadcasted_iota(jnp.int32, (4 * cy, layer), 1)
    which = pr // cy
    wanted = jnp.where(which < 2, which, cz + 1 - which)
    pick = (pc == (pr % cy) * cz + wanted).astype(BF16)
    for x in range(cx):
        rows = dot(pick, c_v[x].reshape(layer, orb)).astype(BF16)
        at = pl.ds(x * cy, cy)
        for side in range(2):
            for k in range(2):
                m = (2 * side + k) * cy
                z_tx[side, k, at] = rows[m : m + cy]
    for copy in push_z:
        copy.start()

    loads[1].wait()
    loads[2].wait()

    blocks = own_s.shape[0]
    owners = [own_s[b] for b in range(blocks)]
    ranks = []
    for b in range(blocks):
        rank = jnp.int32(0)
        for e in range(b):
            rank = rank + (owners[e] == owners[b]).astype(jnp.int32)
        ranks.append(rank)
    for o in range(n_x):
        for k in range(CAP):
            index = jnp.int32(blocks)
            for b in range(blocks):
                index = jnp.where((owners[b] == o) & (ranks[b] == k), b, index)
            sel_s[o * CAP + k] = index
    prod[blocks] = jnp.zeros((orb, orb), BF16)

    lane = lax.broadcasted_iota(jnp.int32, (layer, cz), 1)
    cell = lax.broadcasted_iota(jnp.int32, (layer, cz), 0) % cz
    both = jnp.zeros((orb, 2 * orb), F32)
    for x in range(cx):
        beyond = jnp.zeros((layer, orb), F32)
        for n in (x - 1, x + 1):
            if 0 <= n < cx:
                beyond = beyond + c_v[n].reshape(layer, orb).astype(F32)
        smooth = (dot(stencil, c_v[x].reshape(layer, orb)) + SMOOTH * beyond).astype(BF16)
        s_v[x] = smooth.reshape(cy, cz, orb)
        spread = jnp.broadcast_to(pot_v[x][:, None, :], (cy, cz, cz)).reshape(layer, cz)
        value = jnp.sum(jnp.where(lane == cell, spread, 0.0), axis=1, keepdims=True)
        weighted = (value * smooth.astype(F32)).astype(BF16)
        both = both + gram(smooth, jnp.concatenate([smooth, weighted], axis=1))
        edge = dot(pick, smooth).astype(BF16)
        at = pl.ds(x * cy, cy)
        z_own[0, at] = edge[:cy]
        z_own[1, at] = edge[2 * cy : 3 * cy]
    hamilton = both[:, orb:].astype(BF16)

    c_edge = [
        c_v[0].reshape(layer, orb),
        c_v[cx - 1].reshape(layer, orb),
        c_v[:, 0].reshape(face, orb),
        c_v[:, cy - 1].reshape(face, orb),
        z_tx[0, 0],
        z_tx[1, 0],
    ]
    s_edge = [
        s_v[0].reshape(layer, orb),
        s_v[cx - 1].reshape(layer, orb),
        s_v[:, 0].reshape(face, orb),
        s_v[:, cy - 1].reshape(face, orb),
        z_own[0],
        z_own[1],
    ]
    edges = jnp.zeros((orb, orb), F32)
    for c in c_edge:
        edges = edges + gram(c, c)
    correlation = both[:, :orb] + SMOOTH * SMOOTH * edges
    diagonal = lax.broadcasted_iota(jnp.int32, (orb, orb), 0) == lax.broadcasted_iota(
        jnp.int32, (orb, orb), 1
    )
    scale = math.sqrt(cx * cy * cz)
    unit = jnp.where(diagonal, 1.0, 0.0)
    prod[0] = dot((scale * (correlation - unit)).astype(BF16), hamilton).astype(BF16)

    def multiply(block, deviation):
        prod[block] = dot(deviation, hamilton).astype(BF16)

    def meet(at, c_far, c_deep, matrix):
        s_far = (dot(matrix, c_far) + SMOOTH * c_deep.astype(F32)).astype(BF16)
        mine = jnp.concatenate([s_edge[at], c_edge[at]], axis=0)
        other = jnp.concatenate([c_far, s_far], axis=0)
        factor = scale * SMOOTH
        return (factor * gram(mine, other)).astype(BF16), mine, other, factor

    def turned(mine, other, factor):
        return (factor * gram(other, mine)).astype(BF16)

    push_x.wait_recv()
    deviation, *rest = meet(0, x_rx[1].reshape(layer, orb), x_rx[0].reshape(layer, orb), stencil)
    ret_tx[0] = turned(*rest)
    back_x.start()
    multiply(1, deviation)

    for side in range(2):
        push_z[1 - side].wait_recv()
        deviation, *_ = meet(4 + side, z_rx[side, 0], z_rx[side, 1], small)
        multiply(5 + side, deviation)

    back_x.wait_recv()
    multiply(2, ret_rx[0])

    @pl.when(low)
    def _():
        for side in range(2):
            push_y[1 - side].wait_recv()
            far, deep = (1, 0) if side == 0 else (0, 1)
            deviation, *rest = meet(
                2 + side,
                y_rx[side, :, far].reshape(face, orb),
                y_rx[side, :, deep].reshape(face, orb),
                small,
            )
            ret_tx[1 + side] = turned(*rest)
            back_y[side].start()
            multiply(3 + side, deviation)

    @pl.when(jnp.logical_not(low))
    def _():
        for side in range(2):
            back_y[1 - side].wait_recv()
            multiply(3 + side, ret_rx[1 + side])

    def hand(o):
        return pltpu.make_async_remote_copy(
            src_ref=slots.at[o],
            dst_ref=out.at[pl.ds(CAP * p, CAP)],
            send_sem=a2a_tx.at[o],
            recv_sem=a2a_rx.at[p],
            device_id=(o, q, r),
            device_id_type=MESH,
        )

    for o in range(n_x):

        @pl.when(o != p)
        def _():
            for k in range(CAP):
                slots[o, k] = prod[sel_s[o * CAP + k]]
            hand(o).start()

    for k in range(CAP):
        out[CAP * p + k] = prod[sel_s[CAP * p + k]]

    push_x.wait_send()
    back_x.wait_send()
    for copy in push_z:
        copy.wait_send()

    @pl.when(low)
    def _():
        for copy in back_y:
            copy.wait_send()

    @pl.when(jnp.logical_not(low))
    def _():
        for copy in push_y:
            copy.wait_send()

    for o in range(n_x):

        @pl.when(o != p)
        def _():
            hand(o).wait_send()
            pltpu.make_async_remote_copy(
                src_ref=slots.at[o],
                dst_ref=out.at[pl.ds(CAP * o, CAP)],
                send_sem=a2a_tx.at[o],
                recv_sem=a2a_rx.at[o],
                device_id=(o, q, r),
                device_id_type=MESH,
            ).wait_recv()


def local(coefficients, potential, owner_map):
    sizes = tuple(lax.axis_size(a) for a in ("gx", "gy", "gz"))
    cx, cy, cz, orb = coefficients.shape
    blocks = owner_map.size
    n_x = sizes[0]
    result = pl.pallas_call(
        functools.partial(kernel, sizes),
        out_shape=jax.ShapeDtypeStruct((n_x * CAP, orb, orb), BF16),
        in_specs=[pl.BlockSpec(memory_space=pl.ANY)] * 3,
        out_specs=pl.BlockSpec(memory_space=pltpu.VMEM),
        scratch_shapes=[
            pltpu.VMEM((cx, cy, cz, orb), BF16),
            pltpu.VMEM((cx, cy, cz, orb), BF16),
            pltpu.VMEM((cx, cy, cz), F32),
            pltpu.SMEM((blocks,), jnp.int32),
            pltpu.SMEM((n_x * CAP,), jnp.int32),
            pltpu.VMEM((2, cy, cz, orb), BF16),
            pltpu.VMEM((2, cx, 2, cz, orb), BF16),
            pltpu.VMEM((2, 2, cx * cy, orb), BF16),
            pltpu.VMEM((2, cx * cy, orb), BF16),
            pltpu.VMEM((2, 2, cx * cy, orb), BF16),
            pltpu.VMEM((3, orb, orb), BF16),
            pltpu.VMEM((3, orb, orb), BF16),
            pltpu.VMEM((blocks + 1, orb, orb), BF16),
            pltpu.VMEM((n_x, CAP, orb, orb), BF16),
            pltpu.SemaphoreType.DMA((3,)),
            pltpu.SemaphoreType.DMA((8,)),
            pltpu.SemaphoreType.DMA((8,)),
            pltpu.SemaphoreType.DMA((n_x,)),
            pltpu.SemaphoreType.DMA((n_x,)),
        ],
        compiler_params=pltpu.CompilerParams(
            collective_id=0, has_side_effects=True
        ),
        name="correction",
    )(coefficients, potential, owner_map.reshape(blocks))
    return result.reshape(1, 1, 1, n_x * CAP, orb, orb)


def solution(mesh):
    in_specs = (P("gx", "gy", "gz", None), P("gx", "gy", "gz"), P("gx", "gy", "gz", None, None))
    out_specs = P("gx", "gy", "gz", None, None, None)
    return jax.shard_map(local, mesh=mesh, in_specs=in_specs, out_specs=out_specs, check_vma=False)
```

```python
import functools
import math

import jax
import jax.numpy as jnp
from jax import lax
from jax.experimental import pallas as pl
from jax.experimental.pallas import tpu as pltpu
from jax.sharding import PartitionSpec as P

CAP = 2
SMOOTH = 0.25
MESH = pl.DeviceIdType.MESH
F32 = jnp.float32
BF16 = jnp.bfloat16


def dot(a, b):
    return jnp.dot(a, b, preferred_element_type=F32)


def gram(a, b):
    return lax.dot_general(a, b, (((0,), (0,)), ((), ())), preferred_element_type=F32)


def kernel(
    sizes,
    c_hbm,
    pot_hbm,
    own_hbm,
    out,
    c_v,
    s_v,
    pot_v,
    own_s,
    sel_s,
    x_rx,
    y_rx,
    z_tx,
    z_own,
    z_rx,
    ret_tx,
    ret_rx,
    prod,
    slots,
    load_sem,
    tx_sem,
    rx_sem,
    a2a_tx,
    a2a_rx,
    ready,
):
    n_x, n_y, n_z = sizes
    cx, cy, cz, orb = c_hbm.shape
    p, q, r = (lax.axis_index(a) for a in ("gx", "gy", "gz"))
    low = q % 2 == 0
    x_lo, x_hi = ((p + n_x - 1) % n_x, q, r), ((p + 1) % n_x, q, r)
    y_lo, y_hi = (p, (q + n_y - 1) % n_y, r), (p, (q + 1) % n_y, r)
    z_lo, z_hi = (p, q, (r + n_z - 1) % n_z), (p, q, (r + 1) % n_z)

    loads = [
        pltpu.make_async_copy(c_hbm, c_v, load_sem.at[0]),
        pltpu.make_async_copy(pot_hbm, pot_v, load_sem.at[1]),
        pltpu.make_async_copy(own_hbm, own_s, load_sem.at[2]),
    ]
    for load in loads:
        load.start()

    def made_above(pair):
        return pair < n_x // 2

    up_lo, up_hi = made_above((p + n_x - 1) % n_x), made_above(p)

    barrier = pltpu.get_barrier_semaphore()
    for o in range(1, n_x):

        @pl.when(o > p)
        def _():
            pl.semaphore_signal(barrier, inc=1, device_id=(o, q, r), device_id_type=MESH)

    pl.semaphore_signal(barrier, inc=1, device_id=z_hi, device_id_type=MESH)
    behind = jnp.logical_not(low) & (r % 2 == 1)

    @pl.when(jnp.logical_not(behind))
    def _():
        pl.semaphore_signal(barrier, inc=1, device_id=z_lo, device_id_type=MESH)

    @pl.when(low)
    def _():
        for peer in (y_lo, y_hi):
            pl.semaphore_signal(barrier, inc=1, device_id=peer, device_id_type=MESH)

    def send(src, dst, sem, peer):
        return pltpu.make_async_remote_copy(
            src_ref=src,
            dst_ref=dst,
            send_sem=tx_sem.at[sem],
            recv_sem=rx_sem.at[sem],
            device_id=peer,
            device_id_type=MESH,
        )

    push_x_hi = send(c_v.at[pl.ds(cx - 2, 2)], x_rx.at[0], 0, x_hi)
    push_x_lo = send(c_v.at[pl.ds(0, 2)], x_rx.at[1], 3, x_lo)
    push_z = [send(z_tx.at[0], z_rx.at[1], 1, z_lo), send(z_tx.at[1], z_rx.at[0], 2, z_hi)]
    back_x_lo = send(ret_tx.at[0], ret_rx.at[1], 8, x_lo)
    back_x_hi = send(ret_tx.at[1], ret_rx.at[0], 9, x_hi)
    push_y = [
        send(c_v.at[:, pl.ds(0, 2)], y_rx.at[1], 4, y_lo),
        send(c_v.at[:, pl.ds(cy - 2, 2)], y_rx.at[0], 5, y_hi),
    ]
    back_y = [
        send(ret_tx.at[2], ret_rx.at[3], 6, y_lo),
        send(ret_tx.at[3], ret_rx.at[2], 7, y_hi),
    ]

    loads[0].wait()
    pl.semaphore_wait(barrier, p + jnp.where(low, 2, 4))

    @pl.when(jnp.logical_not(low))
    def _():
        for copy in push_y:
            copy.start()

    @pl.when(behind)
    def _():
        for copy in push_y:
            copy.wait_send()
        pl.semaphore_signal(barrier, inc=1, device_id=z_lo, device_id_type=MESH)

    @pl.when(jnp.logical_not(up_lo) & (p > 0))
    def _():
        push_x_lo.start()

    for o in range(n_x - 1):

        @pl.when(o < p)
        def _():
            which = jnp.where(o == p - 1, 0, jnp.where((o == 0) & (p == n_x - 1), 2, 1))
            pl.semaphore_signal(ready.at[which], inc=1, device_id=(o, q, r), device_id_type=MESH)

    layer = cy * cz
    row = lax.broadcasted_iota(jnp.int32, (layer, layer), 0)
    col = lax.broadcasted_iota(jnp.int32, (layer, layer), 1)
    apart = jnp.abs(row - col)
    beside = ((apart == 1) & (row // cz == col // cz)) | (apart == cz)
    stencil = jnp.where(apart == 0, 1.0, jnp.where(beside, SMOOTH, 0.0)).astype(BF16)
    face = cx * cz
    small = stencil[:face, :face]

    pr = lax.broadcasted_iota(jnp.int32, (4 * cy, layer), 0)
    pc = lax.broadcasted_iota(jnp.int32, (4 * cy, layer), 1)
    which = pr // cy
    wanted = jnp.where(which < 2, which, cz + 1 - which)
    pick = (pc == (pr % cy) * cz + wanted).astype(BF16)
    for x in range(cx):
        rows = dot(pick, c_v[x].reshape(layer, orb)).astype(BF16)
        at = pl.ds(x * cy, cy)
        for side in range(2):
            for k in range(2):
                m = (2 * side + k) * cy
                z_tx[side, k, at] = rows[m : m + cy]
    for copy in push_z:
        copy.start()

    @pl.when(p < n_x - 1)
    def _():
        pl.semaphore_wait(ready.at[0], 1)

    @pl.when(up_hi)
    def _():
        push_x_hi.start()

    loads[1].wait()
    loads[2].wait()

    blocks = own_s.shape[0]
    owners = [own_s[b] for b in range(blocks)]
    ranks = []
    for b in range(blocks):
        rank = jnp.int32(0)
        for e in range(b):
            rank = rank + (owners[e] == owners[b]).astype(jnp.int32)
        ranks.append(rank)
    for o in range(n_x):
        for k in range(CAP):
            index = jnp.int32(blocks)
            for b in range(blocks):
                index = jnp.where((owners[b] == o) & (ranks[b] == k), b, index)
            sel_s[o * CAP + k] = index
    prod[blocks] = jnp.zeros((orb, orb), BF16)

    lane = lax.broadcasted_iota(jnp.int32, (layer, cz), 1)
    cell = lax.broadcasted_iota(jnp.int32, (layer, cz), 0) % cz
    both = jnp.zeros((orb, 2 * orb), F32)
    for x in range(cx):
        beyond = jnp.zeros((layer, orb), F32)
        for n in (x - 1, x + 1):
            if 0 <= n < cx:
                beyond = beyond + c_v[n].reshape(layer, orb).astype(F32)
        smooth = (dot(stencil, c_v[x].reshape(layer, orb)) + SMOOTH * beyond).astype(BF16)
        s_v[x] = smooth.reshape(cy, cz, orb)
        spread = jnp.broadcast_to(pot_v[x][:, None, :], (cy, cz, cz)).reshape(layer, cz)
        value = jnp.sum(jnp.where(lane == cell, spread, 0.0), axis=1, keepdims=True)
        weighted = (value * smooth.astype(F32)).astype(BF16)
        both = both + gram(smooth, jnp.concatenate([smooth, weighted], axis=1))
        edge = dot(pick, smooth).astype(BF16)
        at = pl.ds(x * cy, cy)
        z_own[0, at] = edge[:cy]
        z_own[1, at] = edge[2 * cy : 3 * cy]
    hamilton = both[:, orb:].astype(BF16)

    @pl.when(p == 0)
    def _():
        pl.semaphore_wait(ready.at[2], 1)
        push_x_lo.start()

    c_edge = [
        c_v[0].reshape(layer, orb),
        c_v[cx - 1].reshape(layer, orb),
        c_v[:, 0].reshape(face, orb),
        c_v[:, cy - 1].reshape(face, orb),
        z_tx[0, 0],
        z_tx[1, 0],
    ]
    s_edge = [
        s_v[0].reshape(layer, orb),
        s_v[cx - 1].reshape(layer, orb),
        s_v[:, 0].reshape(face, orb),
        s_v[:, cy - 1].reshape(face, orb),
        z_own[0],
        z_own[1],
    ]
    edges = jnp.zeros((orb, orb), F32)
    for c in c_edge:
        edges = edges + gram(c, c)
    correlation = both[:, :orb] + SMOOTH * SMOOTH * edges
    diagonal = lax.broadcasted_iota(jnp.int32, (orb, orb), 0) == lax.broadcasted_iota(
        jnp.int32, (orb, orb), 1
    )
    scale = math.sqrt(cx * cy * cz)
    unit = jnp.where(diagonal, 1.0, 0.0)
    prod[0] = dot((scale * (correlation - unit)).astype(BF16), hamilton).astype(BF16)

    def multiply(block, deviation):
        prod[block] = dot(deviation, hamilton).astype(BF16)

    def meet(at, c_far, c_deep, matrix):
        s_far = (dot(matrix, c_far) + SMOOTH * c_deep.astype(F32)).astype(BF16)
        mine = jnp.concatenate([s_edge[at], c_edge[at]], axis=0)
        other = jnp.concatenate([c_far, s_far], axis=0)
        factor = scale * SMOOTH
        return (factor * gram(mine, other)).astype(BF16), mine, other, factor

    def turned(mine, other, factor):
        return (factor * gram(other, mine)).astype(BF16)

    @pl.when(up_lo)
    def _():
        push_x_hi.wait_recv()
        deviation, *rest = meet(0, x_rx[0, 1].reshape(layer, orb), x_rx[0, 0].reshape(layer, orb), stencil)
        ret_tx[0] = turned(*rest)
        back_x_lo.start()
        multiply(1, deviation)

    @pl.when(jnp.logical_not(up_hi))
    def _():
        push_x_lo.wait_recv()
        deviation, *rest = meet(1, x_rx[1, 0].reshape(layer, orb), x_rx[1, 1].reshape(layer, orb), stencil)
        ret_tx[1] = turned(*rest)
        back_x_hi.start()
        multiply(2, deviation)

    for side in range(2):
        push_z[1 - side].wait_recv()
        deviation, *_ = meet(4 + side, z_rx[side, 0], z_rx[side, 1], small)
        multiply(5 + side, deviation)

    @pl.when(up_hi)
    def _():
        back_x_lo.wait_recv()
        multiply(2, ret_rx[1])

    @pl.when(jnp.logical_not(up_lo))
    def _():
        back_x_hi.wait_recv()
        multiply(1, ret_rx[0])

    @pl.when(low)
    def _():
        for side in range(2):
            push_y[1 - side].wait_recv()
            far, deep = (1, 0) if side == 0 else (0, 1)
            deviation, *rest = meet(
                2 + side,
                y_rx[side, :, far].reshape(face, orb),
                y_rx[side, :, deep].reshape(face, orb),
                small,
            )
            ret_tx[2 + side] = turned(*rest)
            back_y[side].start()
            multiply(3 + side, deviation)

    @pl.when(jnp.logical_not(low))
    def _():
        for side in range(2):
            back_y[1 - side].wait_recv()
            multiply(3 + side, ret_rx[2 + side])

    @pl.when(p < n_x - 2)
    def _():
        pl.semaphore_wait(ready.at[1], n_x - 2 - p - jnp.where(p == 0, 1, 0))

    def hand(o):
        return pltpu.make_async_remote_copy(
            src_ref=slots.at[o],
            dst_ref=out.at[pl.ds(CAP * p, CAP)],
            send_sem=a2a_tx.at[o],
            recv_sem=a2a_rx.at[p],
            device_id=(o, q, r),
            device_id_type=MESH,
        )

    for o in range(n_x):

        @pl.when(o != p)
        def _():
            for k in range(CAP):
                slots[o, k] = prod[sel_s[o * CAP + k]]
            hand(o).start()

    for k in range(CAP):
        out[CAP * p + k] = prod[sel_s[CAP * p + k]]

    for copy in push_z:
        copy.wait_send()

    @pl.when(up_hi)
    def _():
        push_x_hi.wait_send()

    @pl.when(jnp.logical_not(up_hi))
    def _():
        back_x_hi.wait_send()

    @pl.when(up_lo)
    def _():
        back_x_lo.wait_send()

    @pl.when(jnp.logical_not(up_lo))
    def _():
        push_x_lo.wait_send()

    @pl.when(jnp.logical_not(low) & jnp.logical_not(behind))
    def _():
        for copy in push_y:
            copy.wait_send()

    @pl.when(low)
    def _():
        for copy in back_y:
            copy.wait_send()

    for o in range(n_x):

        @pl.when(o != p)
        def _():
            hand(o).wait_send()
            pltpu.make_async_remote_copy(
                src_ref=slots.at[o],
                dst_ref=out.at[pl.ds(CAP * o, CAP)],
                send_sem=a2a_tx.at[o],
                recv_sem=a2a_rx.at[o],
                device_id=(o, q, r),
                device_id_type=MESH,
            ).wait_recv()


def local(coefficients, potential, owner_map):
    sizes = tuple(lax.axis_size(a) for a in ("gx", "gy", "gz"))
    cx, cy, cz, orb = coefficients.shape
    blocks = owner_map.size
    n_x = sizes[0]
    result = pl.pallas_call(
        functools.partial(kernel, sizes),
        out_shape=jax.ShapeDtypeStruct((n_x * CAP, orb, orb), BF16),
        in_specs=[pl.BlockSpec(memory_space=pl.ANY)] * 3,
        out_specs=pl.BlockSpec(memory_space=pltpu.VMEM),
        scratch_shapes=[
            pltpu.VMEM((cx, cy, cz, orb), BF16),
            pltpu.VMEM((cx, cy, cz, orb), BF16),
            pltpu.VMEM((cx, cy, cz), F32),
            pltpu.SMEM((blocks,), jnp.int32),
            pltpu.SMEM((n_x * CAP,), jnp.int32),
            pltpu.VMEM((2, 2, cy, cz, orb), BF16),
            pltpu.VMEM((2, cx, 2, cz, orb), BF16),
            pltpu.VMEM((2, 2, cx * cy, orb), BF16),
            pltpu.VMEM((2, cx * cy, orb), BF16),
            pltpu.VMEM((2, 2, cx * cy, orb), BF16),
            pltpu.VMEM((4, orb, orb), BF16),
            pltpu.VMEM((4, orb, orb), BF16),
            pltpu.VMEM((blocks + 1, orb, orb), BF16),
            pltpu.VMEM((n_x, CAP, orb, orb), BF16),
            pltpu.SemaphoreType.DMA((3,)),
            pltpu.SemaphoreType.DMA((10,)),
            pltpu.SemaphoreType.DMA((10,)),
            pltpu.SemaphoreType.DMA((n_x,)),
            pltpu.SemaphoreType.DMA((n_x,)),
            pltpu.SemaphoreType.REGULAR((3,)),
        ],
        compiler_params=pltpu.CompilerParams(
            collective_id=0, has_side_effects=True, vmem_limit_bytes=53 * 1024 * 1024
        ),
        name="correction",
    )(coefficients, potential, owner_map.reshape(blocks))
    return result.reshape(1, 1, 1, n_x * CAP, orb, orb)


def solution(mesh):
    in_specs = (P("gx", "gy", "gz", None), P("gx", "gy", "gz"), P("gx", "gy", "gz", None, None))
    out_specs = P("gx", "gy", "gz", None, None, None)
    return jax.shard_map(local, mesh=mesh, in_specs=in_specs, out_specs=out_specs, check_vma=False)
```

```python
import functools
import math

import jax
import jax.numpy as jnp
from jax import lax
from jax.experimental import pallas as pl
from jax.experimental.pallas import tpu as pltpu
from jax.sharding import PartitionSpec as P

CAP = 2
SMOOTH = 0.25
MESH = pl.DeviceIdType.MESH
F32 = jnp.float32
BF16 = jnp.bfloat16


def dot(a, b):
    return jnp.dot(a, b, preferred_element_type=F32)


def gram(a, b):
    return lax.dot_general(a, b, (((0,), (0,)), ((), ())), preferred_element_type=F32)


def kernel(
    sizes,
    c_hbm,
    pot_hbm,
    own_hbm,
    out,
    c_v,
    s_v,
    pot_v,
    own_s,
    sel_s,
    x_rx,
    y_rx,
    z_tx,
    z_own,
    z_rx,
    ret_tx,
    ret_rx,
    prod,
    slots,
    load_sem,
    tx_sem,
    rx_sem,
    a2a_tx,
    a2a_rx,
    ready,
    go,
):
    n_x, n_y, n_z = sizes
    cx, cy, cz, orb = c_hbm.shape
    p, q, r = (lax.axis_index(a) for a in ("gx", "gy", "gz"))
    low = q % 2 == 0
    x_lo, x_hi = ((p + n_x - 1) % n_x, q, r), ((p + 1) % n_x, q, r)
    y_lo, y_hi = (p, (q + n_y - 1) % n_y, r), (p, (q + 1) % n_y, r)
    z_lo, z_hi = (p, q, (r + n_z - 1) % n_z), (p, q, (r + 1) % n_z)

    loads = [
        pltpu.make_async_copy(c_hbm, c_v, load_sem.at[0]),
        pltpu.make_async_copy(pot_hbm, pot_v, load_sem.at[1]),
        pltpu.make_async_copy(own_hbm, own_s, load_sem.at[2]),
    ]
    for load in loads:
        load.start()

    def made_above(pair):
        return pair < n_x // 2

    up_lo, up_hi = made_above((p + n_x - 1) % n_x), made_above(p)

    barrier = pltpu.get_barrier_semaphore()
    for o in range(1, n_x):

        @pl.when(o > p)
        def _():
            pl.semaphore_signal(barrier, inc=1, device_id=(o, q, r), device_id_type=MESH)

    for peer in (z_lo, z_hi):
        pl.semaphore_signal(barrier, inc=1, device_id=peer, device_id_type=MESH)

    even = p % 2 == 0
    first = jnp.logical_not(low) & (r % 2 == 1)
    second = jnp.logical_not(low) & (r % 2 == 0)
    for o in range(2, n_x, 2):

        @pl.when(second & even & (o > p))
        def _():
            pl.semaphore_signal(barrier, inc=1, device_id=(o, q, z_hi[2]), device_id_type=MESH)

    @pl.when(low)
    def _():
        for peer in (y_lo, y_hi):
            pl.semaphore_signal(barrier, inc=1, device_id=peer, device_id_type=MESH)

    def send(src, dst, sem, peer):
        return pltpu.make_async_remote_copy(
            src_ref=src,
            dst_ref=dst,
            send_sem=tx_sem.at[sem],
            recv_sem=rx_sem.at[sem],
            device_id=peer,
            device_id_type=MESH,
        )

    push_x_hi = send(c_v.at[pl.ds(cx - 2, 2)], x_rx.at[0], 0, x_hi)
    push_x_lo = send(c_v.at[pl.ds(0, 2)], x_rx.at[1], 3, x_lo)
    push_z = [send(z_tx.at[0], z_rx.at[1], 1, z_lo), send(z_tx.at[1], z_rx.at[0], 2, z_hi)]
    back_x_lo = send(ret_tx.at[0], ret_rx.at[1], 8, x_lo)
    back_x_hi = send(ret_tx.at[1], ret_rx.at[0], 9, x_hi)
    push_y = [
        send(c_v.at[:, pl.ds(0, 2)], y_rx.at[1], 4, y_lo),
        send(c_v.at[:, pl.ds(cy - 2, 2)], y_rx.at[0], 5, y_hi),
    ]
    back_y = [
        send(ret_tx.at[2], ret_rx.at[3], 6, y_lo),
        send(ret_tx.at[3], ret_rx.at[2], 7, y_hi),
    ]

    pl.semaphore_wait(barrier, p + jnp.where(low, 2, 4) + jnp.where(first & even, p // 2, 0))

    for o in range(n_x - 1):

        @pl.when(o < p)
        def _():
            which = jnp.where(o == p - 1, 0, jnp.where((o == 0) & (p == n_x - 1), 2, 1))
            pl.semaphore_signal(ready.at[which], inc=1, device_id=(o, q, r), device_id_type=MESH)

    loads[0].wait()

    @pl.when(first)
    def _():
        for copy in reversed(push_y):
            copy.start()

    @pl.when(jnp.logical_not(up_lo) & (p > 0))
    def _():
        push_x_lo.start()

    layer = cy * cz
    row = lax.broadcasted_iota(jnp.int32, (layer, layer), 0)
    col = lax.broadcasted_iota(jnp.int32, (layer, layer), 1)
    apart = jnp.abs(row - col)
    beside = ((apart == 1) & (row // cz == col // cz)) | (apart == cz)
    stencil = jnp.where(apart == 0, 1.0, jnp.where(beside, SMOOTH, 0.0)).astype(BF16)
    face = cx * cz
    small = stencil[:face, :face]

    pr = lax.broadcasted_iota(jnp.int32, (4 * cy, layer), 0)
    pc = lax.broadcasted_iota(jnp.int32, (4 * cy, layer), 1)
    which = pr // cy
    wanted = jnp.where(which < 2, which, cz + 1 - which)
    pick = (pc == (pr % cy) * cz + wanted).astype(BF16)
    for x in range(cx):
        rows = dot(pick, c_v[x].reshape(layer, orb)).astype(BF16)
        at = pl.ds(x * cy, cy)
        for side in range(2):
            for k in range(2):
                m = (2 * side + k) * cy
                z_tx[side, k, at] = rows[m : m + cy]
    for copy in push_z:
        copy.start()

    @pl.when(first)
    def _():
        for copy in push_y:
            copy.wait_send()
        for o in range(n_x):

            @pl.when((o == p) | (even & (o % 2 == 0) & (o < p)))
            def _():
                pl.semaphore_signal(go, inc=1, device_id=(o, q, z_lo[2]), device_id_type=MESH)

    @pl.when(p < n_x - 1)
    def _():
        pl.semaphore_wait(ready.at[0], 1)

    @pl.when(up_hi)
    def _():
        push_x_hi.start()

    @pl.when(second)
    def _():
        pl.semaphore_wait(go, jnp.where(even, (n_x - p + 1) // 2, 1))
        for copy in reversed(push_y):
            copy.start()

    loads[1].wait()
    loads[2].wait()

    blocks = own_s.shape[0]
    owners = [own_s[b] for b in range(blocks)]
    ranks = []
    for b in range(blocks):
        rank = jnp.int32(0)
        for e in range(b):
            rank = rank + (owners[e] == owners[b]).astype(jnp.int32)
        ranks.append(rank)
    for o in range(n_x):
        for k in range(CAP):
            index = jnp.int32(blocks)
            for b in range(blocks):
                index = jnp.where((owners[b] == o) & (ranks[b] == k), b, index)
            sel_s[o * CAP + k] = index
    prod[blocks] = jnp.zeros((orb, orb), BF16)

    lane = lax.broadcasted_iota(jnp.int32, (layer, cz), 1)
    cell = lax.broadcasted_iota(jnp.int32, (layer, cz), 0) % cz
    both = jnp.zeros((orb, 2 * orb), F32)
    for x in range(cx):
        beyond = jnp.zeros((layer, orb), F32)
        for n in (x - 1, x + 1):
            if 0 <= n < cx:
                beyond = beyond + c_v[n].reshape(layer, orb).astype(F32)
        smooth = (dot(stencil, c_v[x].reshape(layer, orb)) + SMOOTH * beyond).astype(BF16)
        s_v[x] = smooth.reshape(cy, cz, orb)
        spread = jnp.broadcast_to(pot_v[x][:, None, :], (cy, cz, cz)).reshape(layer, cz)
        value = jnp.sum(jnp.where(lane == cell, spread, 0.0), axis=1, keepdims=True)
        weighted = (value * smooth.astype(F32)).astype(BF16)
        both = both + gram(smooth, jnp.concatenate([smooth, weighted], axis=1))
        edge = dot(pick, smooth).astype(BF16)
        at = pl.ds(x * cy, cy)
        z_own[0, at] = edge[:cy]
        z_own[1, at] = edge[2 * cy : 3 * cy]
    hamilton = both[:, orb:].astype(BF16)

    @pl.when(p == 0)
    def _():
        pl.semaphore_wait(ready.at[2], 1)
        push_x_lo.start()

    c_edge = [
        c_v[0].reshape(layer, orb),
        c_v[cx - 1].reshape(layer, orb),
        c_v[:, 0].reshape(face, orb),
        c_v[:, cy - 1].reshape(face, orb),
        z_tx[0, 0],
        z_tx[1, 0],
    ]
    s_edge = [
        s_v[0].reshape(layer, orb),
        s_v[cx - 1].reshape(layer, orb),
        s_v[:, 0].reshape(face, orb),
        s_v[:, cy - 1].reshape(face, orb),
        z_own[0],
        z_own[1],
    ]
    edges = jnp.zeros((orb, orb), F32)
    for c in c_edge:
        edges = edges + gram(c, c)
    correlation = both[:, :orb] + SMOOTH * SMOOTH * edges
    diagonal = lax.broadcasted_iota(jnp.int32, (orb, orb), 0) == lax.broadcasted_iota(
        jnp.int32, (orb, orb), 1
    )
    scale = math.sqrt(cx * cy * cz)
    unit = jnp.where(diagonal, 1.0, 0.0)
    prod[0] = dot((scale * (correlation - unit)).astype(BF16), hamilton).astype(BF16)

    def multiply(block, deviation):
        prod[block] = dot(deviation, hamilton).astype(BF16)

    def meet(at, c_far, c_deep, matrix):
        s_far = (dot(matrix, c_far) + SMOOTH * c_deep.astype(F32)).astype(BF16)
        mine = jnp.concatenate([s_edge[at], c_edge[at]], axis=0)
        other = jnp.concatenate([c_far, s_far], axis=0)
        factor = scale * SMOOTH
        return (factor * gram(mine, other)).astype(BF16), mine, other, factor

    def turned(mine, other, factor):
        return (factor * gram(other, mine)).astype(BF16)

    @pl.when(up_lo)
    def _():
        push_x_hi.wait_recv()
        deviation, *rest = meet(0, x_rx[0, 1].reshape(layer, orb), x_rx[0, 0].reshape(layer, orb), stencil)
        ret_tx[0] = turned(*rest)
        back_x_lo.start()
        multiply(1, deviation)

    @pl.when(jnp.logical_not(up_hi))
    def _():
        push_x_lo.wait_recv()
        deviation, *rest = meet(1, x_rx[1, 0].reshape(layer, orb), x_rx[1, 1].reshape(layer, orb), stencil)
        ret_tx[1] = turned(*rest)
        back_x_hi.start()
        multiply(2, deviation)

    for side in range(2):
        push_z[1 - side].wait_recv()
        deviation, *_ = meet(4 + side, z_rx[side, 0], z_rx[side, 1], small)
        multiply(5 + side, deviation)

    @pl.when(up_hi)
    def _():
        back_x_lo.wait_recv()
        multiply(2, ret_rx[1])

    @pl.when(jnp.logical_not(up_lo))
    def _():
        back_x_hi.wait_recv()
        multiply(1, ret_rx[0])

    @pl.when(low)
    def _():
        for side in range(2):
            push_y[1 - side].wait_recv()
            far, deep = (1, 0) if side == 0 else (0, 1)
            deviation, *rest = meet(
                2 + side,
                y_rx[side, :, far].reshape(face, orb),
                y_rx[side, :, deep].reshape(face, orb),
                small,
            )
            ret_tx[2 + side] = turned(*rest)
            back_y[side].start()
            multiply(3 + side, deviation)

    @pl.when(jnp.logical_not(low))
    def _():
        for side in range(2):
            back_y[1 - side].wait_recv()
            multiply(3 + side, ret_rx[2 + side])

    @pl.when(p < n_x - 2)
    def _():
        pl.semaphore_wait(ready.at[1], n_x - 2 - p - jnp.where(p == 0, 1, 0))

    def hand(o):
        return pltpu.make_async_remote_copy(
            src_ref=slots.at[o],
            dst_ref=out.at[pl.ds(CAP * p, CAP)],
            send_sem=a2a_tx.at[o],
            recv_sem=a2a_rx.at[p],
            device_id=(o, q, r),
            device_id_type=MESH,
        )

    for o in range(n_x):

        @pl.when(o != p)
        def _():
            for k in range(CAP):
                slots[o, k] = prod[sel_s[o * CAP + k]]
            hand(o).start()

    for k in range(CAP):
        out[CAP * p + k] = prod[sel_s[CAP * p + k]]

    for copy in push_z:
        copy.wait_send()

    @pl.when(up_hi)
    def _():
        push_x_hi.wait_send()

    @pl.when(jnp.logical_not(up_hi))
    def _():
        back_x_hi.wait_send()

    @pl.when(up_lo)
    def _():
        back_x_lo.wait_send()

    @pl.when(jnp.logical_not(up_lo))
    def _():
        push_x_lo.wait_send()

    @pl.when(second)
    def _():
        for copy in push_y:
            copy.wait_send()

    @pl.when(low)
    def _():
        for copy in back_y:
            copy.wait_send()

    for o in range(n_x):

        @pl.when(o != p)
        def _():
            hand(o).wait_send()
            pltpu.make_async_remote_copy(
                src_ref=slots.at[o],
                dst_ref=out.at[pl.ds(CAP * o, CAP)],
                send_sem=a2a_tx.at[o],
                recv_sem=a2a_rx.at[o],
                device_id=(o, q, r),
                device_id_type=MESH,
            ).wait_recv()


def local(coefficients, potential, owner_map):
    sizes = tuple(lax.axis_size(a) for a in ("gx", "gy", "gz"))
    cx, cy, cz, orb = coefficients.shape
    blocks = owner_map.size
    n_x = sizes[0]
    result = pl.pallas_call(
        functools.partial(kernel, sizes),
        out_shape=jax.ShapeDtypeStruct((n_x * CAP, orb, orb), BF16),
        in_specs=[pl.BlockSpec(memory_space=pl.ANY)] * 3,
        out_specs=pl.BlockSpec(memory_space=pltpu.VMEM),
        scratch_shapes=[
            pltpu.VMEM((cx, cy, cz, orb), BF16),
            pltpu.VMEM((cx, cy, cz, orb), BF16),
            pltpu.VMEM((cx, cy, cz), F32),
            pltpu.SMEM((blocks,), jnp.int32),
            pltpu.SMEM((n_x * CAP,), jnp.int32),
            pltpu.VMEM((2, 2, cy, cz, orb), BF16),
            pltpu.VMEM((2, cx, 2, cz, orb), BF16),
            pltpu.VMEM((2, 2, cx * cy, orb), BF16),
            pltpu.VMEM((2, cx * cy, orb), BF16),
            pltpu.VMEM((2, 2, cx * cy, orb), BF16),
            pltpu.VMEM((4, orb, orb), BF16),
            pltpu.VMEM((4, orb, orb), BF16),
            pltpu.VMEM((blocks + 1, orb, orb), BF16),
            pltpu.VMEM((n_x, CAP, orb, orb), BF16),
            pltpu.SemaphoreType.DMA((3,)),
            pltpu.SemaphoreType.DMA((10,)),
            pltpu.SemaphoreType.DMA((10,)),
            pltpu.SemaphoreType.DMA((n_x,)),
            pltpu.SemaphoreType.DMA((n_x,)),
            pltpu.SemaphoreType.REGULAR((3,)),
            pltpu.SemaphoreType.REGULAR,
        ],
        compiler_params=pltpu.CompilerParams(
            collective_id=0, has_side_effects=True, vmem_limit_bytes=53 * 1024 * 1024
        ),
        name="correction",
    )(coefficients, potential, owner_map.reshape(blocks))
    return result.reshape(1, 1, 1, n_x * CAP, orb, orb)


def solution(mesh):
    in_specs = (P("gx", "gy", "gz", None), P("gx", "gy", "gz"), P("gx", "gy", "gz", None, None))
    out_specs = P("gx", "gy", "gz", None, None, None)
    return jax.shard_map(local, mesh=mesh, in_specs=in_specs, out_specs=out_specs, check_vma=False)
```

```python
import functools
import math

import jax
import jax.numpy as jnp
from jax import lax
from jax.experimental import pallas as pl
from jax.experimental.pallas import tpu as pltpu
from jax.sharding import PartitionSpec as P

CAP = 2
SMOOTH = 0.25
MESH = pl.DeviceIdType.MESH
F32 = jnp.float32
BF16 = jnp.bfloat16


def dot(a, b):
    return jnp.dot(a, b, preferred_element_type=F32)


def gram(a, b):
    return lax.dot_general(a, b, (((0,), (0,)), ((), ())), preferred_element_type=F32)


def kernel(
    sizes,
    c_hbm,
    pot_hbm,
    own_hbm,
    out,
    c_v,
    s_v,
    pot_v,
    own_s,
    sel_s,
    x_rx,
    y_rx,
    z_tx,
    z_own,
    z_rx,
    ret_tx,
    ret_rx,
    prod,
    slots,
    load_sem,
    tx_sem,
    rx_sem,
    a2a_tx,
    a2a_rx,
    ready,
    go,
    relayed,
    relay_ok,
    relay_tx,
    relay_rx,
):
    n_x, n_y, n_z = sizes
    cx, cy, cz, orb = c_hbm.shape
    p, q, r = (lax.axis_index(a) for a in ("gx", "gy", "gz"))
    low = q % 2 == 0
    x_lo, x_hi = ((p + n_x - 1) % n_x, q, r), ((p + 1) % n_x, q, r)
    y_lo, y_hi = (p, (q + n_y - 1) % n_y, r), (p, (q + 1) % n_y, r)
    z_lo, z_hi = (p, q, (r + n_z - 1) % n_z), (p, q, (r + 1) % n_z)

    loads = [
        pltpu.make_async_copy(c_hbm, c_v, load_sem.at[0]),
        pltpu.make_async_copy(pot_hbm, pot_v, load_sem.at[1]),
        pltpu.make_async_copy(own_hbm, own_s, load_sem.at[2]),
    ]
    for load in loads:
        load.start()

    def made_above(pair):
        return pair < n_x // 2

    up_lo, up_hi = made_above((p + n_x - 1) % n_x), made_above(p)

    barrier = pltpu.get_barrier_semaphore()
    for o in range(1, n_x):

        @pl.when(o > p)
        def _():
            pl.semaphore_signal(barrier, inc=1, device_id=(o, q, r), device_id_type=MESH)

    for peer in (z_lo, z_hi):
        pl.semaphore_signal(barrier, inc=1, device_id=peer, device_id_type=MESH)

    even = p % 2 == 0
    first = jnp.logical_not(low) & (r % 2 == 1)
    second = jnp.logical_not(low) & (r % 2 == 0)
    for o in range(2, n_x, 2):

        @pl.when(second & even & (o > p))
        def _():
            pl.semaphore_signal(barrier, inc=1, device_id=(o, q, z_hi[2]), device_id_type=MESH)

    @pl.when(low)
    def _():
        for peer in (y_lo, y_hi):
            pl.semaphore_signal(barrier, inc=1, device_id=peer, device_id_type=MESH)

    def send(src, dst, sem, peer):
        return pltpu.make_async_remote_copy(
            src_ref=src,
            dst_ref=dst,
            send_sem=tx_sem.at[sem],
            recv_sem=rx_sem.at[sem],
            device_id=peer,
            device_id_type=MESH,
        )

    push_x_hi = send(c_v.at[pl.ds(cx - 2, 2)], x_rx.at[0], 0, x_hi)
    push_x_lo = send(c_v.at[pl.ds(0, 2)], x_rx.at[1], 3, x_lo)
    push_z = [send(z_tx.at[0], z_rx.at[1], 1, z_lo), send(z_tx.at[1], z_rx.at[0], 2, z_hi)]
    back_x_lo = send(ret_tx.at[0], ret_rx.at[1], 8, x_lo)
    back_x_hi = send(ret_tx.at[1], ret_rx.at[0], 9, x_hi)
    push_y = [
        send(c_v.at[:, pl.ds(0, 2)], y_rx.at[1], 4, y_lo),
        send(c_v.at[:, pl.ds(cy - 2, 2)], y_rx.at[0], 5, y_hi),
    ]
    back_y = [
        send(ret_tx.at[2], ret_rx.at[3], 6, y_lo),
        send(ret_tx.at[3], ret_rx.at[2], 7, y_hi),
    ]

    last, middle = n_x - 1, n_x // 2
    routed = low & (p == last)
    relay = jnp.logical_not(low) & (p == middle)

    @pl.when(low & ((p < 2) | (p == last)))
    def _():
        peer = (middle, y_hi[1], r)
        pl.semaphore_signal(barrier, inc=1, device_id=peer, device_id_type=MESH)

    known = p + jnp.where(low, 2, 4) + jnp.where(first & even, p // 2, 0)
    pl.semaphore_wait(barrier, known + jnp.where(relay, 3, 0))

    @pl.when(relay)
    def _():
        peer = (last, y_lo[1], r)
        pl.semaphore_signal(relay_ok, inc=1, device_id=peer, device_id_type=MESH)

    for o in range(n_x - 1):

        @pl.when(o < p)
        def _():
            which = jnp.where(o == p - 1, 0, jnp.where((o == 0) & (p == n_x - 1), 2, 1))
            pl.semaphore_signal(ready.at[which], inc=1, device_id=(o, q, r), device_id_type=MESH)

    loads[0].wait()

    @pl.when(first)
    def _():
        for copy in reversed(push_y):
            copy.start()

    @pl.when(jnp.logical_not(up_lo) & (p > 0))
    def _():
        push_x_lo.start()

    layer = cy * cz
    row = lax.broadcasted_iota(jnp.int32, (layer, layer), 0)
    col = lax.broadcasted_iota(jnp.int32, (layer, layer), 1)
    apart = jnp.abs(row - col)
    beside = ((apart == 1) & (row // cz == col // cz)) | (apart == cz)
    stencil = jnp.where(apart == 0, 1.0, jnp.where(beside, SMOOTH, 0.0)).astype(BF16)
    face = cx * cz
    small = stencil[:face, :face]

    pr = lax.broadcasted_iota(jnp.int32, (4 * cy, layer), 0)
    pc = lax.broadcasted_iota(jnp.int32, (4 * cy, layer), 1)
    which = pr // cy
    wanted = jnp.where(which < 2, which, cz + 1 - which)
    pick = (pc == (pr % cy) * cz + wanted).astype(BF16)
    for x in range(cx):
        rows = dot(pick, c_v[x].reshape(layer, orb)).astype(BF16)
        at = pl.ds(x * cy, cy)
        for side in range(2):
            for k in range(2):
                m = (2 * side + k) * cy
                z_tx[side, k, at] = rows[m : m + cy]
    for copy in push_z:
        copy.start()

    @pl.when(first)
    def _():
        for copy in push_y:
            copy.wait_send()
        for o in range(n_x):

            @pl.when((o == p) | (even & (o % 2 == 0) & (o < p) & (p < n_x - 2)))
            def _():
                pl.semaphore_signal(go, inc=1, device_id=(o, q, z_lo[2]), device_id_type=MESH)

    @pl.when(p < n_x - 1)
    def _():
        pl.semaphore_wait(ready.at[0], 1)

    @pl.when(up_hi)
    def _():
        push_x_hi.start()

    @pl.when(second)
    def _():
        pl.semaphore_wait(go, jnp.where(even & (p < n_x - 2), (n_x - 1 - p) // 2, 1))
        for copy in reversed(push_y):
            copy.start()

    loads[1].wait()
    loads[2].wait()

    blocks = own_s.shape[0]
    owners = [own_s[b] for b in range(blocks)]
    ranks = []
    for b in range(blocks):
        rank = jnp.int32(0)
        for e in range(b):
            rank = rank + (owners[e] == owners[b]).astype(jnp.int32)
        ranks.append(rank)
    for o in range(n_x):
        for k in range(CAP):
            index = jnp.int32(blocks)
            for b in range(blocks):
                index = jnp.where((owners[b] == o) & (ranks[b] == k), b, index)
            sel_s[o * CAP + k] = index
    prod[blocks] = jnp.zeros((orb, orb), BF16)

    lane = lax.broadcasted_iota(jnp.int32, (layer, cz), 1)
    cell = lax.broadcasted_iota(jnp.int32, (layer, cz), 0) % cz
    both = jnp.zeros((orb, 2 * orb), F32)
    for x in range(cx):
        beyond = jnp.zeros((layer, orb), F32)
        for n in (x - 1, x + 1):
            if 0 <= n < cx:
                beyond = beyond + c_v[n].reshape(layer, orb).astype(F32)
        smooth = (dot(stencil, c_v[x].reshape(layer, orb)) + SMOOTH * beyond).astype(BF16)
        s_v[x] = smooth.reshape(cy, cz, orb)
        spread = jnp.broadcast_to(pot_v[x][:, None, :], (cy, cz, cz)).reshape(layer, cz)
        value = jnp.sum(jnp.where(lane == cell, spread, 0.0), axis=1, keepdims=True)
        weighted = (value * smooth.astype(F32)).astype(BF16)
        both = both + gram(smooth, jnp.concatenate([smooth, weighted], axis=1))
        edge = dot(pick, smooth).astype(BF16)
        at = pl.ds(x * cy, cy)
        z_own[0, at] = edge[:cy]
        z_own[1, at] = edge[2 * cy : 3 * cy]
    hamilton = both[:, orb:].astype(BF16)

    @pl.when(p == 0)
    def _():
        pl.semaphore_wait(ready.at[2], 1)
        push_x_lo.start()

    c_edge = [
        c_v[0].reshape(layer, orb),
        c_v[cx - 1].reshape(layer, orb),
        c_v[:, 0].reshape(face, orb),
        c_v[:, cy - 1].reshape(face, orb),
        z_tx[0, 0],
        z_tx[1, 0],
    ]
    s_edge = [
        s_v[0].reshape(layer, orb),
        s_v[cx - 1].reshape(layer, orb),
        s_v[:, 0].reshape(face, orb),
        s_v[:, cy - 1].reshape(face, orb),
        z_own[0],
        z_own[1],
    ]
    edges = jnp.zeros((orb, orb), F32)
    for c in c_edge:
        edges = edges + gram(c, c)
    correlation = both[:, :orb] + SMOOTH * SMOOTH * edges
    diagonal = lax.broadcasted_iota(jnp.int32, (orb, orb), 0) == lax.broadcasted_iota(
        jnp.int32, (orb, orb), 1
    )
    scale = math.sqrt(cx * cy * cz)
    unit = jnp.where(diagonal, 1.0, 0.0)
    prod[0] = dot((scale * (correlation - unit)).astype(BF16), hamilton).astype(BF16)

    def multiply(block, deviation):
        prod[block] = dot(deviation, hamilton).astype(BF16)

    def meet(at, c_far, c_deep, matrix):
        s_far = (dot(matrix, c_far) + SMOOTH * c_deep.astype(F32)).astype(BF16)
        mine = jnp.concatenate([s_edge[at], c_edge[at]], axis=0)
        other = jnp.concatenate([c_far, s_far], axis=0)
        factor = scale * SMOOTH
        return (factor * gram(mine, other)).astype(BF16), mine, other, factor

    def turned(mine, other, factor):
        return (factor * gram(other, mine)).astype(BF16)

    @pl.when(up_lo)
    def _():
        push_x_hi.wait_recv()
        deviation, *rest = meet(0, x_rx[0, 1].reshape(layer, orb), x_rx[0, 0].reshape(layer, orb), stencil)
        ret_tx[0] = turned(*rest)
        back_x_lo.start()
        multiply(1, deviation)

    @pl.when(jnp.logical_not(up_hi))
    def _():
        push_x_lo.wait_recv()
        deviation, *rest = meet(1, x_rx[1, 0].reshape(layer, orb), x_rx[1, 1].reshape(layer, orb), stencil)
        ret_tx[1] = turned(*rest)
        back_x_hi.start()
        multiply(2, deviation)

    for side in range(2):
        push_z[1 - side].wait_recv()
        deviation, *_ = meet(4 + side, z_rx[side, 0], z_rx[side, 1], small)
        multiply(5 + side, deviation)

    @pl.when(up_hi)
    def _():
        back_x_lo.wait_recv()
        multiply(2, ret_rx[1])

    @pl.when(jnp.logical_not(up_lo))
    def _():
        back_x_hi.wait_recv()
        multiply(1, ret_rx[0])

    @pl.when(low)
    def _():
        for side in range(2):
            push_y[1 - side].wait_recv()
            far, deep = (1, 0) if side == 0 else (0, 1)
            deviation, *rest = meet(
                2 + side,
                y_rx[side, :, far].reshape(face, orb),
                y_rx[side, :, deep].reshape(face, orb),
                small,
            )
            ret_tx[2 + side] = turned(*rest)
            back_y[side].start()
            multiply(3 + side, deviation)

    def to_relay(o):
        return pltpu.make_async_remote_copy(
            src_ref=slots.at[o],
            dst_ref=relayed.at[o],
            send_sem=a2a_tx.at[o],
            recv_sem=relay_rx.at[o],
            device_id=(middle, y_hi[1], r),
            device_id_type=MESH,
        )

    def from_relay(o):
        return pltpu.make_async_remote_copy(
            src_ref=relayed.at[o],
            dst_ref=out.at[pl.ds(CAP * last, CAP)],
            send_sem=relay_tx.at[o],
            recv_sem=a2a_rx.at[last],
            device_id=(o, y_lo[1], r),
            device_id_type=MESH,
        )

    @pl.when(relay)
    def _():
        for o in range(2):
            to_relay(o).wait_recv()
            from_relay(o).start()

    @pl.when(jnp.logical_not(low))
    def _():
        for side in range(2):
            back_y[1 - side].wait_recv()
            multiply(3 + side, ret_rx[2 + side])

    @pl.when(p < n_x - 2)
    def _():
        pl.semaphore_wait(ready.at[1], n_x - 2 - p - jnp.where(p == 0, 1, 0))

    def hand(o):
        return pltpu.make_async_remote_copy(
            src_ref=slots.at[o],
            dst_ref=out.at[pl.ds(CAP * p, CAP)],
            send_sem=a2a_tx.at[o],
            recv_sem=a2a_rx.at[p],
            device_id=(o, q, r),
            device_id_type=MESH,
        )

    @pl.when(routed)
    def _():
        pl.semaphore_wait(relay_ok, 1)
        for o in range(2):
            for k in range(CAP):
                slots[o, k] = prod[sel_s[o * CAP + k]]
            to_relay(o).start()

    for o in range(n_x):

        @pl.when((o != p) & jnp.logical_not(routed & (o < 2)))
        def _():
            for k in range(CAP):
                slots[o, k] = prod[sel_s[o * CAP + k]]
            hand(o).start()

    for k in range(CAP):
        out[CAP * p + k] = prod[sel_s[CAP * p + k]]

    for copy in push_z:
        copy.wait_send()

    @pl.when(relay)
    def _():
        for o in range(2):
            from_relay(o).wait_send()

    @pl.when(up_hi)
    def _():
        push_x_hi.wait_send()

    @pl.when(jnp.logical_not(up_hi))
    def _():
        back_x_hi.wait_send()

    @pl.when(up_lo)
    def _():
        back_x_lo.wait_send()

    @pl.when(jnp.logical_not(up_lo))
    def _():
        push_x_lo.wait_send()

    @pl.when(second)
    def _():
        for copy in push_y:
            copy.wait_send()

    @pl.when(low)
    def _():
        for copy in back_y:
            copy.wait_send()

    for o in range(n_x):

        @pl.when(o != p)
        def _():
            hand(o).wait_send()
            pltpu.make_async_remote_copy(
                src_ref=slots.at[o],
                dst_ref=out.at[pl.ds(CAP * o, CAP)],
                send_sem=a2a_tx.at[o],
                recv_sem=a2a_rx.at[o],
                device_id=(o, q, r),
                device_id_type=MESH,
            ).wait_recv()


def local(coefficients, potential, owner_map):
    sizes = tuple(lax.axis_size(a) for a in ("gx", "gy", "gz"))
    cx, cy, cz, orb = coefficients.shape
    blocks = owner_map.size
    n_x = sizes[0]
    result = pl.pallas_call(
        functools.partial(kernel, sizes),
        out_shape=jax.ShapeDtypeStruct((n_x * CAP, orb, orb), BF16),
        in_specs=[pl.BlockSpec(memory_space=pl.ANY)] * 3,
        out_specs=pl.BlockSpec(memory_space=pltpu.VMEM),
        scratch_shapes=[
            pltpu.VMEM((cx, cy, cz, orb), BF16),
            pltpu.VMEM((cx, cy, cz, orb), BF16),
            pltpu.VMEM((cx, cy, cz), F32),
            pltpu.SMEM((blocks,), jnp.int32),
            pltpu.SMEM((n_x * CAP,), jnp.int32),
            pltpu.VMEM((2, 2, cy, cz, orb), BF16),
            pltpu.VMEM((2, cx, 2, cz, orb), BF16),
            pltpu.VMEM((2, 2, cx * cy, orb), BF16),
            pltpu.VMEM((2, cx * cy, orb), BF16),
            pltpu.VMEM((2, 2, cx * cy, orb), BF16),
            pltpu.VMEM((4, orb, orb), BF16),
            pltpu.VMEM((4, orb, orb), BF16),
            pltpu.VMEM((blocks + 1, orb, orb), BF16),
            pltpu.VMEM((n_x, CAP, orb, orb), BF16),
            pltpu.SemaphoreType.DMA((3,)),
            pltpu.SemaphoreType.DMA((10,)),
            pltpu.SemaphoreType.DMA((10,)),
            pltpu.SemaphoreType.DMA((n_x,)),
            pltpu.SemaphoreType.DMA((n_x,)),
            pltpu.SemaphoreType.REGULAR((3,)),
            pltpu.SemaphoreType.REGULAR,
            pltpu.VMEM((2, CAP, orb, orb), BF16),
            pltpu.SemaphoreType.REGULAR,
            pltpu.SemaphoreType.DMA((2,)),
            pltpu.SemaphoreType.DMA((2,)),
        ],
        compiler_params=pltpu.CompilerParams(
            collective_id=0, has_side_effects=True, vmem_limit_bytes=53 * 1024 * 1024
        ),
        name="correction",
    )(coefficients, potential, owner_map.reshape(blocks))
    return result.reshape(1, 1, 1, n_x * CAP, orb, orb)


def solution(mesh):
    in_specs = (P("gx", "gy", "gz", None), P("gx", "gy", "gz"), P("gx", "gy", "gz", None, None))
    out_specs = P("gx", "gy", "gz", None, None, None)
    return jax.shard_map(local, mesh=mesh, in_specs=in_specs, out_specs=out_specs, check_vma=False)
```

```python
import functools
import math

import jax
import jax.numpy as jnp
from jax import lax
from jax.experimental import pallas as pl
from jax.experimental.pallas import tpu as pltpu
from jax.sharding import PartitionSpec as P

CAP = 2
SMOOTH = 0.25
MESH = pl.DeviceIdType.MESH
F32 = jnp.float32
BF16 = jnp.bfloat16


def dot(a, b):
    return jnp.dot(a, b, preferred_element_type=F32)


def gram(a, b):
    return lax.dot_general(a, b, (((0,), (0,)), ((), ())), preferred_element_type=F32)


def kernel(
    sizes,
    c_hbm,
    pot_hbm,
    own_hbm,
    out,
    c_v,
    s_v,
    pot_v,
    own_s,
    sel_s,
    x_rx,
    y_rx,
    z_tx,
    z_own,
    z_rx,
    ret_tx,
    ret_rx,
    prod,
    slots,
    load_sem,
    tx_sem,
    rx_sem,
    a2a_tx,
    a2a_rx,
    ready,
    go,
    relayed,
    relay_ok,
    relay_tx,
    relay_rx,
):
    n_x, n_y, n_z = sizes
    cx, cy, cz, orb = c_hbm.shape
    p, q, r = (lax.axis_index(a) for a in ("gx", "gy", "gz"))
    low = q % 2 == 0
    x_lo, x_hi = ((p + n_x - 1) % n_x, q, r), ((p + 1) % n_x, q, r)
    y_lo, y_hi = (p, (q + n_y - 1) % n_y, r), (p, (q + 1) % n_y, r)
    z_lo, z_hi = (p, q, (r + n_z - 1) % n_z), (p, q, (r + 1) % n_z)

    loads = [
        pltpu.make_async_copy(c_hbm, c_v, load_sem.at[0]),
        pltpu.make_async_copy(pot_hbm, pot_v, load_sem.at[1]),
        pltpu.make_async_copy(own_hbm, own_s, load_sem.at[2]),
    ]
    for load in loads:
        load.start()

    def made_above(pair):
        return pair < n_x // 2

    up_lo, up_hi = made_above((p + n_x - 1) % n_x), made_above(p)

    barrier = pltpu.get_barrier_semaphore()
    for o in range(1, n_x):

        @pl.when(o > p)
        def _():
            pl.semaphore_signal(barrier, inc=1, device_id=(o, q, r), device_id_type=MESH)

    beside_z = ((z_lo, r == 0), (z_hi, r < n_z - 1))
    for peer, higher in beside_z:

        @pl.when(low | higher)
        def _():
            pl.semaphore_signal(barrier, inc=1, device_id=peer, device_id_type=MESH)

    even = p % 2 == 0
    first = jnp.logical_not(low) & (r % 2 == 1)
    second = jnp.logical_not(low) & (r % 2 == 0)
    for o in range(2, n_x, 2):

        @pl.when(second & even & (o > p))
        def _():
            pl.semaphore_signal(barrier, inc=1, device_id=(o, q, z_hi[2]), device_id_type=MESH)

    @pl.when(low)
    def _():
        for peer in (y_lo, y_hi):
            pl.semaphore_signal(barrier, inc=1, device_id=peer, device_id_type=MESH)

    def send(src, dst, sem, peer):
        return pltpu.make_async_remote_copy(
            src_ref=src,
            dst_ref=dst,
            send_sem=tx_sem.at[sem],
            recv_sem=rx_sem.at[sem],
            device_id=peer,
            device_id_type=MESH,
        )

    push_x_hi = send(c_v.at[pl.ds(cx - 2, 2)], x_rx.at[0], 0, x_hi)
    push_x_lo = send(c_v.at[pl.ds(0, 2)], x_rx.at[1], 3, x_lo)
    push_z = [send(z_tx.at[0], z_rx.at[1], 1, z_lo), send(z_tx.at[1], z_rx.at[0], 2, z_hi)]
    back_x_lo = send(ret_tx.at[0], ret_rx.at[1], 8, x_lo)
    back_x_hi = send(ret_tx.at[1], ret_rx.at[0], 9, x_hi)
    push_y = [
        send(c_v.at[:, pl.ds(0, 2)], y_rx.at[1], 4, y_lo),
        send(c_v.at[:, pl.ds(cy - 2, 2)], y_rx.at[0], 5, y_hi),
    ]
    back_y = [
        send(ret_tx.at[2], ret_rx.at[3], 6, y_lo),
        send(ret_tx.at[3], ret_rx.at[2], 7, y_hi),
    ]

    last, middle = n_x - 1, n_x // 2
    routed = low & (p == last)
    relay = jnp.logical_not(low) & (p == middle)

    @pl.when(low & ((p < 2) | (p == last)))
    def _():
        peer = (middle, y_hi[1], r)
        pl.semaphore_signal(barrier, inc=1, device_id=peer, device_id_type=MESH)

    lower_z = jnp.where(r == 0, 0, jnp.where(r == n_z - 1, 2, 1))
    known = p + 2 + jnp.where(low, 0, lower_z) + jnp.where(first & even, p // 2, 0)
    pl.semaphore_wait(barrier, known + jnp.where(relay, 3, 0))

    @pl.when(relay)
    def _():
        peer = (last, y_lo[1], r)
        pl.semaphore_signal(relay_ok, inc=1, device_id=peer, device_id_type=MESH)

    for o in range(n_x - 1):

        @pl.when(o < p)
        def _():
            which = jnp.where(o == p - 1, 0, jnp.where((o == 0) & (p == n_x - 1), 2, 1))
            pl.semaphore_signal(ready.at[which], inc=1, device_id=(o, q, r), device_id_type=MESH)

    for peer, higher in beside_z:

        @pl.when(jnp.logical_not(low | higher))
        def _():
            pl.semaphore_signal(ready.at[3], inc=1, device_id=peer, device_id_type=MESH)

    loads[0].wait()

    @pl.when(first)
    def _():
        for copy in reversed(push_y):
            copy.start()

    @pl.when(jnp.logical_not(up_lo) & (p > 0))
    def _():
        push_x_lo.start()

    layer = cy * cz
    row = lax.broadcasted_iota(jnp.int32, (layer, layer), 0)
    col = lax.broadcasted_iota(jnp.int32, (layer, layer), 1)
    apart = jnp.abs(row - col)
    beside = ((apart == 1) & (row // cz == col // cz)) | (apart == cz)
    stencil = jnp.where(apart == 0, 1.0, jnp.where(beside, SMOOTH, 0.0)).astype(BF16)
    face = cx * cz
    small = stencil[:face, :face]

    pr = lax.broadcasted_iota(jnp.int32, (4 * cy, layer), 0)
    pc = lax.broadcasted_iota(jnp.int32, (4 * cy, layer), 1)
    which = pr // cy
    wanted = jnp.where(which < 2, which, cz + 1 - which)
    pick = (pc == (pr % cy) * cz + wanted).astype(BF16)
    for x in range(cx):
        rows = dot(pick, c_v[x].reshape(layer, orb)).astype(BF16)
        at = pl.ds(x * cy, cy)
        for side in range(2):
            for k in range(2):
                m = (2 * side + k) * cy
                z_tx[side, k, at] = rows[m : m + cy]
    @pl.when(jnp.logical_not(low) & (r < n_z - 1))
    def _():
        pl.semaphore_wait(ready.at[3], jnp.where(r == 0, 2, 1))

    for copy in push_z:
        copy.start()

    @pl.when(first)
    def _():
        for copy in push_y:
            copy.wait_send()
        for o in range(n_x):

            @pl.when((o == p) | (even & (o % 2 == 0) & (o < p) & (p < n_x - 2)))
            def _():
                pl.semaphore_signal(go, inc=1, device_id=(o, q, z_lo[2]), device_id_type=MESH)

    @pl.when(p < n_x - 1)
    def _():
        pl.semaphore_wait(ready.at[0], 1)

    @pl.when(up_hi)
    def _():
        push_x_hi.start()

    @pl.when(second)
    def _():
        pl.semaphore_wait(go, jnp.where(even & (p < n_x - 2), (n_x - 1 - p) // 2, 1))
        for copy in reversed(push_y):
            copy.start()

    loads[1].wait()
    loads[2].wait()

    blocks = own_s.shape[0]
    owners = [own_s[b] for b in range(blocks)]
    ranks = []
    for b in range(blocks):
        rank = jnp.int32(0)
        for e in range(b):
            rank = rank + (owners[e] == owners[b]).astype(jnp.int32)
        ranks.append(rank)
    for o in range(n_x):
        for k in range(CAP):
            index = jnp.int32(blocks)
            for b in range(blocks):
                index = jnp.where((owners[b] == o) & (ranks[b] == k), b, index)
            sel_s[o * CAP + k] = index
    prod[blocks] = jnp.zeros((orb, orb), BF16)

    lane = lax.broadcasted_iota(jnp.int32, (layer, cz), 1)
    cell = lax.broadcasted_iota(jnp.int32, (layer, cz), 0) % cz
    both = jnp.zeros((orb, 2 * orb), F32)
    for x in range(cx):
        beyond = jnp.zeros((layer, orb), F32)
        for n in (x - 1, x + 1):
            if 0 <= n < cx:
                beyond = beyond + c_v[n].reshape(layer, orb).astype(F32)
        smooth = (dot(stencil, c_v[x].reshape(layer, orb)) + SMOOTH * beyond).astype(BF16)
        s_v[x] = smooth.reshape(cy, cz, orb)
        spread = jnp.broadcast_to(pot_v[x][:, None, :], (cy, cz, cz)).reshape(layer, cz)
        value = jnp.sum(jnp.where(lane == cell, spread, 0.0), axis=1, keepdims=True)
        weighted = (value * smooth.astype(F32)).astype(BF16)
        both = both + gram(smooth, jnp.concatenate([smooth, weighted], axis=1))
        edge = dot(pick, smooth).astype(BF16)
        at = pl.ds(x * cy, cy)
        z_own[0, at] = edge[:cy]
        z_own[1, at] = edge[2 * cy : 3 * cy]
    hamilton = both[:, orb:].astype(BF16)

    @pl.when(p == 0)
    def _():
        pl.semaphore_wait(ready.at[2], 1)
        push_x_lo.start()

    c_edge = [
        c_v[0].reshape(layer, orb),
        c_v[cx - 1].reshape(layer, orb),
        c_v[:, 0].reshape(face, orb),
        c_v[:, cy - 1].reshape(face, orb),
        z_tx[0, 0],
        z_tx[1, 0],
    ]
    s_edge = [
        s_v[0].reshape(layer, orb),
        s_v[cx - 1].reshape(layer, orb),
        s_v[:, 0].reshape(face, orb),
        s_v[:, cy - 1].reshape(face, orb),
        z_own[0],
        z_own[1],
    ]
    edges = jnp.zeros((orb, orb), F32)
    for c in c_edge:
        edges = edges + gram(c, c)
    correlation = both[:, :orb] + SMOOTH * SMOOTH * edges
    diagonal = lax.broadcasted_iota(jnp.int32, (orb, orb), 0) == lax.broadcasted_iota(
        jnp.int32, (orb, orb), 1
    )
    scale = math.sqrt(cx * cy * cz)
    unit = jnp.where(diagonal, 1.0, 0.0)
    prod[0] = dot((scale * (correlation - unit)).astype(BF16), hamilton).astype(BF16)

    def multiply(block, deviation):
        prod[block] = dot(deviation, hamilton).astype(BF16)

    def meet(at, c_far, c_deep, matrix):
        s_far = (dot(matrix, c_far) + SMOOTH * c_deep.astype(F32)).astype(BF16)
        mine = jnp.concatenate([s_edge[at], c_edge[at]], axis=0)
        other = jnp.concatenate([c_far, s_far], axis=0)
        factor = scale * SMOOTH
        return (factor * gram(mine, other)).astype(BF16), mine, other, factor

    def turned(mine, other, factor):
        return (factor * gram(other, mine)).astype(BF16)

    @pl.when(up_lo)
    def _():
        push_x_hi.wait_recv()
        deviation, *rest = meet(0, x_rx[0, 1].reshape(layer, orb), x_rx[0, 0].reshape(layer, orb), stencil)
        ret_tx[0] = turned(*rest)
        back_x_lo.start()
        multiply(1, deviation)

    @pl.when(jnp.logical_not(up_hi))
    def _():
        push_x_lo.wait_recv()
        deviation, *rest = meet(1, x_rx[1, 0].reshape(layer, orb), x_rx[1, 1].reshape(layer, orb), stencil)
        ret_tx[1] = turned(*rest)
        back_x_hi.start()
        multiply(2, deviation)

    for side in range(2):
        push_z[1 - side].wait_recv()
        deviation, *_ = meet(4 + side, z_rx[side, 0], z_rx[side, 1], small)
        multiply(5 + side, deviation)

    @pl.when(up_hi)
    def _():
        back_x_lo.wait_recv()
        multiply(2, ret_rx[1])

    @pl.when(jnp.logical_not(up_lo))
    def _():
        back_x_hi.wait_recv()
        multiply(1, ret_rx[0])

    @pl.when(low)
    def _():
        for side in range(2):
            push_y[1 - side].wait_recv()
            far, deep = (1, 0) if side == 0 else (0, 1)
            deviation, *rest = meet(
                2 + side,
                y_rx[side, :, far].reshape(face, orb),
                y_rx[side, :, deep].reshape(face, orb),
                small,
            )
            ret_tx[2 + side] = turned(*rest)
            back_y[side].start()
            multiply(3 + side, deviation)

    def to_relay(o):
        return pltpu.make_async_remote_copy(
            src_ref=slots.at[o],
            dst_ref=relayed.at[o],
            send_sem=a2a_tx.at[o],
            recv_sem=relay_rx.at[o],
            device_id=(middle, y_hi[1], r),
            device_id_type=MESH,
        )

    def from_relay(o):
        return pltpu.make_async_remote_copy(
            src_ref=relayed.at[o],
            dst_ref=out.at[pl.ds(CAP * last, CAP)],
            send_sem=relay_tx.at[o],
            recv_sem=a2a_rx.at[last],
            device_id=(o, y_lo[1], r),
            device_id_type=MESH,
        )

    @pl.when(relay)
    def _():
        for o in range(2):
            to_relay(o).wait_recv()
            from_relay(o).start()

    @pl.when(jnp.logical_not(low))
    def _():
        for side in range(2):
            back_y[1 - side].wait_recv()
            multiply(3 + side, ret_rx[2 + side])

    @pl.when(p < n_x - 2)
    def _():
        pl.semaphore_wait(ready.at[1], n_x - 2 - p - jnp.where(p == 0, 1, 0))

    def hand(o):
        return pltpu.make_async_remote_copy(
            src_ref=slots.at[o],
            dst_ref=out.at[pl.ds(CAP * p, CAP)],
            send_sem=a2a_tx.at[o],
            recv_sem=a2a_rx.at[p],
            device_id=(o, q, r),
            device_id_type=MESH,
        )

    @pl.when(routed)
    def _():
        pl.semaphore_wait(relay_ok, 1)
        for o in range(2):
            for k in range(CAP):
                slots[o, k] = prod[sel_s[o * CAP + k]]
            to_relay(o).start()

    for o in range(n_x):

        @pl.when((o != p) & jnp.logical_not(routed & (o < 2)))
        def _():
            for k in range(CAP):
                slots[o, k] = prod[sel_s[o * CAP + k]]
            hand(o).start()

    for k in range(CAP):
        out[CAP * p + k] = prod[sel_s[CAP * p + k]]

    for copy in push_z:
        copy.wait_send()

    @pl.when(relay)
    def _():
        for o in range(2):
            from_relay(o).wait_send()

    @pl.when(up_hi)
    def _():
        push_x_hi.wait_send()

    @pl.when(jnp.logical_not(up_hi))
    def _():
        back_x_hi.wait_send()

    @pl.when(up_lo)
    def _():
        back_x_lo.wait_send()

    @pl.when(jnp.logical_not(up_lo))
    def _():
        push_x_lo.wait_send()

    @pl.when(second)
    def _():
        for copy in push_y:
            copy.wait_send()

    @pl.when(low)
    def _():
        for copy in back_y:
            copy.wait_send()

    for o in range(n_x):

        @pl.when(o != p)
        def _():
            hand(o).wait_send()
            pltpu.make_async_remote_copy(
                src_ref=slots.at[o],
                dst_ref=out.at[pl.ds(CAP * o, CAP)],
                send_sem=a2a_tx.at[o],
                recv_sem=a2a_rx.at[o],
                device_id=(o, q, r),
                device_id_type=MESH,
            ).wait_recv()


def local(coefficients, potential, owner_map):
    sizes = tuple(lax.axis_size(a) for a in ("gx", "gy", "gz"))
    cx, cy, cz, orb = coefficients.shape
    blocks = owner_map.size
    n_x = sizes[0]
    result = pl.pallas_call(
        functools.partial(kernel, sizes),
        out_shape=jax.ShapeDtypeStruct((n_x * CAP, orb, orb), BF16),
        in_specs=[pl.BlockSpec(memory_space=pl.ANY)] * 3,
        out_specs=pl.BlockSpec(memory_space=pltpu.VMEM),
        scratch_shapes=[
            pltpu.VMEM((cx, cy, cz, orb), BF16),
            pltpu.VMEM((cx, cy, cz, orb), BF16),
            pltpu.VMEM((cx, cy, cz), F32),
            pltpu.SMEM((blocks,), jnp.int32),
            pltpu.SMEM((n_x * CAP,), jnp.int32),
            pltpu.VMEM((2, 2, cy, cz, orb), BF16),
            pltpu.VMEM((2, cx, 2, cz, orb), BF16),
            pltpu.VMEM((2, 2, cx * cy, orb), BF16),
            pltpu.VMEM((2, cx * cy, orb), BF16),
            pltpu.VMEM((2, 2, cx * cy, orb), BF16),
            pltpu.VMEM((4, orb, orb), BF16),
            pltpu.VMEM((4, orb, orb), BF16),
            pltpu.VMEM((blocks + 1, orb, orb), BF16),
            pltpu.VMEM((n_x, CAP, orb, orb), BF16),
            pltpu.SemaphoreType.DMA((3,)),
            pltpu.SemaphoreType.DMA((10,)),
            pltpu.SemaphoreType.DMA((10,)),
            pltpu.SemaphoreType.DMA((n_x,)),
            pltpu.SemaphoreType.DMA((n_x,)),
            pltpu.SemaphoreType.REGULAR((4,)),
            pltpu.SemaphoreType.REGULAR,
            pltpu.VMEM((2, CAP, orb, orb), BF16),
            pltpu.SemaphoreType.REGULAR,
            pltpu.SemaphoreType.DMA((2,)),
            pltpu.SemaphoreType.DMA((2,)),
        ],
        compiler_params=pltpu.CompilerParams(
            collective_id=0, has_side_effects=True, vmem_limit_bytes=53 * 1024 * 1024
        ),
        name="correction",
    )(coefficients, potential, owner_map.reshape(blocks))
    return result.reshape(1, 1, 1, n_x * CAP, orb, orb)


def solution(mesh):
    in_specs = (P("gx", "gy", "gz", None), P("gx", "gy", "gz"), P("gx", "gy", "gz", None, None))
    out_specs = P("gx", "gy", "gz", None, None, None)
    return jax.shard_map(local, mesh=mesh, in_specs=in_specs, out_specs=out_specs, check_vma=False)
```
